512 devices in a mesh: segment: 16 (over z_hi, y, core), dp: 32 (over x, z_lo).
Axes of the slice: x: 4, y: 4, z: 16 (z_hi: 2, z_lo: 8; z = z_hi * 8 + z_lo), core: 2. Of those that a mesh axis runs over, the one named last changes fastest.
Arguments:
- token_ids: int32 [4096], P('dp'), may hold values from 0 to 152063, as said below
- table: bfloat16 [19008, 28672], P('segment', 'dp'), may hold values from -6 to 6
- out_grad: bfloat16 [4096, 3584], P('dp', 'segment'), may hold values from -6 to 6
Outputs:
- embedded: bfloat16 [4096, 3584], P('dp')
- table_grad: bfloat16 [19008, 28672], P('segment', 'dp')
The draws below stay inside these ranges and needn't reach their ends.
Inputs may be any that keep to these rules, and one draw needn't show every extreme that they name: `token_ids`: in the 128 tokens of each data group, at most 16 ids lie in one segment's slice of 9504 rows with one residue modulo 8; in every data group some segment and residue has exactly 16.
All inputs are finite; a program needn't handle non-finite values.
Results may differ from the reference program's by a relative error of at most 0.001.
Values may be sent and summed in bfloat16 or wider, within the bound.
A program may use at most 64 MiB of HBM per device.

```python
import jax
import jax.numpy as jnp
from jax import lax

D = 3584
ROWS_SECTION = 9504
PACK = 8
TOK_DEV = 128
VOCAB = 152064
TOKENS = 4096


def draw_token_ids(key, part):
    groups = TOKENS // TOK_DEV
    segments = VOCAB // ROWS_SECTION
    buckets = segments * PACK
    capacity = TOK_DEV // PACK
    lines = ROWS_SECTION // PACK
    global_hot = jax.random.randint(jax.random.fold_in(key, 11), (), 0, buckets)

    def one_group(group):
        group_key = jax.random.fold_in(key, 100 + group)
        keys = jax.random.split(group_key, 7)
        order = jax.random.permutation(keys[0], buckets)
        use_global = jax.random.randint(keys[1], (), 0, 2)
        hot = jnp.where(use_global == 1, global_hot, order[0])
        hot_pos = jnp.argmax(order == hot)
        order = order.at[hot_pos].set(order[0]).at[0].set(hot)
        spread = jax.random.randint(keys[2], (), 7, buckets)
        position = jnp.arange(TOK_DEV)
        bucket = jnp.where(position < capacity, order[0], order[1 + (position - capacity) % spread])
        hot_line = jax.random.randint(keys[3], (TOK_DEV,), 0, min(lines, 4))
        any_line = jax.random.randint(keys[4], (TOK_DEV,), 0, lines)
        pick = jax.random.randint(keys[5], (TOK_DEV,), 0, 2)
        line = jnp.where(pick == 1, hot_line, any_line)
        ids = bucket // PACK * ROWS_SECTION + line * PACK + bucket % PACK
        shuffle = jax.random.permutation(keys[6], TOK_DEV)
        return ids[shuffle]
    return jax.vmap(one_group)(jnp.arange(groups)).reshape(-1).astype(jnp.int32)


def shard_levels(rng, dims, cuts, least, top_value):
    level = 1.0
    for axis_at, shards_of in cuts:
        draws = jax.random.uniform(jax.random.fold_in(jax.random.fold_in(rng, 6), axis_at), (shards_of,), jnp.float32, least / len(cuts), top_value / len(cuts))
        level = level * jnp.repeat(jnp.exp(draws), dims[axis_at] // shards_of).reshape((-1,) + (1,) * (len(dims) - 1 - axis_at))
    return level


def normal_values(own_key, shape, deviation, most, cuts=(), held_as=jnp.bfloat16):
    drawn = jax.random.normal(own_key, shape, jnp.float32) * deviation
    if len(cuts) > 0:
        drawn = shard_levels(own_key, shape, cuts, -0.22, 0.18) * drawn
    return jnp.clip(drawn, min=-most, max=most).astype(held_as)


def setup_inputs(seed: int = 0) -> dict:
    splits = jax.random.split(jax.random.key(seed), 4)
    token_ids = draw_token_ids(jax.random.fold_in(splits[3], 71), 0)
    table = normal_values(splits[1], (VOCAB // PACK, PACK * D), 1.0, 6.0, ((0, 16), (1, 32)))
    out_grad = normal_values(splits[2], (TOKENS, D), 1.0, 6.0, ((0, 32), (1, 16)))
    return {"token_ids": token_ids, "table": table, "out_grad": out_grad}


def reference(token_ids, table, out_grad):
    flat = table.reshape(VOCAB, D)
    embedded = jnp.take(flat, token_ids, axis=0)
    width = 128 if D % 128 == 0 else D
    blocks = D // width
    pieces = out_grad.reshape(TOKENS, blocks, width).transpose(1, 0, 2)

    def accumulate(piece):
        total = jnp.zeros((VOCAB, width), jnp.float32).at[token_ids].add(piece.astype(jnp.float32))
        return total.astype(jnp.bfloat16)

    summed = lax.map(accumulate, pieces)
    table_grad = summed.transpose(1, 0, 2).reshape(VOCAB // PACK, PACK * D)
    return embedded, table_grad
```

```python
import functools

import jax
import jax.numpy as jnp
from jax import lax
from jax.experimental import pallas as pl
from jax.experimental.pallas import tpu as pltpu
from jax.sharding import PartitionSpec as P

PACK = 8
BF = jnp.bfloat16
F32 = jnp.float32
MESH = pl.DeviceIdType.MESH

X, Y, Z, ZL = 4, 4, 16, 8
LANE = 128


def place(x, y, z, c):
    return {"segment": (z // ZL) * ZL + y * 2 + c, "dp": x * ZL + z % ZL}


def remote(src, dst, send, recv, peer):
    return pltpu.make_async_remote_copy(
        src_ref=src, dst_ref=dst, send_sem=send, recv_sem=recv,
        device_id=peer, device_id_type=MESH,
    )


def signal(sem, peer):
    pl.semaphore_signal(sem, inc=1, device_id=peer, device_id_type=MESH)


def ring(d, n):
    return min(d % n, n - d % n)


def choose(ids, first, span, slot, cap):
    rows, tok = ids.shape
    local = ids - first
    owned = (local >= 0) & (local < span) & ((ids & (PACK - 1)) == slot)
    before = lax.broadcasted_iota(jnp.int32, (tok, tok), 0) < lax.broadcasted_iota(
        jnp.int32, (tok, tok), 1
    )
    rank = jnp.dot(
        jnp.where(owned, 1.0, 0.0).astype(BF),
        jnp.where(before, 1.0, 0.0).astype(BF),
        preferred_element_type=F32,
    )
    want = lax.broadcasted_iota(jnp.int32, (rows, tok), 0) % cap
    return owned & (rank.astype(jnp.int32) == want), local


def kernel(
    ids_ref, table_ref, grad_ref,
    emb_ref, back_ref, hot_ref,
    ids_all, ids_wide, table, grad, raw_out, raw, rows_out, rows_in, pick, scatter,
    part, halves, sums, zin, back_out,
    load_sem, ids_sem, raw_sem, twin_sem, fwd_sem, half_sem, z_sem, bwd_sem, ag_sem, rel_sem,
):
    seg = lax.axis_index("segment")
    dp = lax.axis_index("dp")
    c = seg % 2
    y = (seg // 2) % Y
    zh = seg // ZL
    zl = dp % ZL
    z = zh * ZL + zl
    x = dp // ZL
    mine = x * Y + y
    k = 2 * y + c
    lines, width = table.shape
    tok = ids_ref.shape[1]
    feat = grad.shape[1]
    groups = X * ZL
    cap = rows_in.shape[3]
    blocks = width // LANE
    span = lines * PACK
    twin = place(x, y, z, 1 - c)

    ids_offs = sorted(
        [(dx, dz) for dx in range(X) for dz in range(-4, 4) if (dx, dz) != (0, 0)],
        key=lambda d: -(ring(d[0], X) + abs(d[1])),
    )
    z_offs = sorted(range(1, Z), key=lambda d: -ring(d, Z))
    far_offs = [d for d in z_offs if not (d <= 3 or d >= Z - 4)]
    plane_offs = sorted(
        [(dx, dy) for dx in range(X) for dy in range(Y) if (dx, dy) != (0, 0)],
        key=lambda d: -(ring(d[0], X) + ring(d[1], Y)),
    )

    def at_z(d):
        return place(x, y, (z + d + Z) % Z, c)

    def at_ids(dx, dz):
        return place((x + dx + X) % X, y, (z + dz + Z) % Z, c)

    def at_plane(dx, dy):
        return place((x + dx + X) % X, (y + dy + Y) % Y, z, c)

    q_out = zh * 2 + y // 2
    raw_y = zl // 2
    raw_to = [(q_out + 4 * a) % Z for a in range(4)]
    raw_self = [(raw_y == y) & (raw_to[a] == z) for a in range(4)]
    q_in = z % 4
    raw_from = []
    for h in range(2):
        for m in range(2):
            raw_from.append(((q_in % 2) * 2 + h, (q_in // 2) * ZL + 2 * y + m))
    from_self = [(fy == y) & (fz == z) for fy, fz in raw_from]

    load_grad = pltpu.make_async_copy(grad_ref, grad, load_sem.at[0])
    load_grad.start()
    load = pltpu.make_async_copy(table_ref, table, load_sem.at[1])
    load.start()

    barrier = pltpu.get_barrier_semaphore()
    signal(barrier, twin)
    for d in far_offs:
        signal(barrier, at_z(-d))
    for dx, dz in ids_offs:
        signal(barrier, at_ids(-dx, -dz))
    for dx, dy in plane_offs:
        signal(barrier, at_plane(-dx, -dy))
    for n, (fy, fz) in enumerate(raw_from):
        @pl.when(jnp.logical_not(from_self[n]))
        def _():
            signal(barrier, place(x, fy, fz, c))
    n_self = jnp.where((raw_y == y) & (z % 4 == q_out), 1, 0)

    eye = lax.broadcasted_iota(jnp.int32, (feat, feat), 0) == lax.broadcasted_iota(
        jnp.int32, (feat, feat), 1
    )
    load_grad.wait()
    raw_out[...] = lax.dot_general(
        jnp.where(eye, 1.0, 0.0).astype(BF), grad[...], (((1,), (1,)), ((), ())),
        preferred_element_type=F32,
    ).astype(BF)
    ids_all[dp] = ids_ref[...]
    pl.semaphore_wait(
        barrier, 1 + len(far_offs) + len(ids_offs) + len(plane_offs) + 4 - n_self
    )

    ids_copies = []
    for n, (dx, dz) in enumerate(ids_offs):
        copy = remote(
            ids_ref, ids_all.at[dp], ids_sem.at[0, n], ids_sem.at[1, n], at_ids(dx, dz)
        )
        copy.start()
        ids_copies.append(copy)

    raw_slot = (y % 2) * 2 + zl % 2
    raw_row = pl.multiple_of(((y % 2) * 2 + c) * feat, 16)
    raw_copies = []
    for a in range(4):
        copy = remote(
            raw_out, raw.at[zl % 2, pl.ds(raw_row, feat)],
            raw_sem.at[0, a], raw_sem.at[1, raw_slot],
            place(x, raw_y, raw_to[a], c),
        )
        raw_copies.append(copy)

        @pl.when(jnp.logical_not(raw_self[a]))
        def _(copy=copy):
            copy.start()

        @pl.when(raw_self[a])
        def _():
            raw[zl % 2, pl.ds(raw_row, feat)] = raw_out[...]

    for copy in ids_copies:
        copy.wait_recv()

    for g in range(groups):
        ids_wide[g] = jnp.broadcast_to(ids_all[g], (cap, tok))
    named, local = choose(
        ids_wide[...].reshape(groups * cap, tok), seg * span, span, dp // (groups // PACK), cap
    )
    line = jnp.sum(
        jnp.where(named, (local // PACK + 1).astype(F32), 0.0), axis=1, keepdims=True
    ).astype(jnp.int32) - 1
    hot_ref[...] = jnp.where(
        lax.broadcasted_iota(jnp.int32, (groups * cap, lines), 1) == line, 1.0, 0.0
    ).astype(BF)
    load.wait()

    cuts = [(0, 4), (4, blocks)]
    fwd = []
    for p, (lo, hi) in enumerate(cuts):
        got = jnp.dot(
            hot_ref[...], table[:, lo * LANE:hi * LANE], preferred_element_type=F32
        ).astype(BF)
        for g in range(groups):
            gx, j = g // ZL, g % ZL
            for b in range(lo, hi):
                core = (j - b) % ZL
                rows_out[gx * Y + core // 2, b, core % 2] = got[
                    g * cap:(g + 1) * cap, (b - lo) * LANE:(b - lo + 1) * LANE
                ]
        sent = []
        for n, (dx, dy) in enumerate(plane_offs):
            to = ((x + dx) % X) * Y + (y + dy) % Y
            copy = remote(
                rows_out.at[to, pl.ds(lo, hi - lo)], rows_in.at[mine, pl.ds(lo, hi - lo)],
                fwd_sem.at[0, n, p], fwd_sem.at[1, n, p], at_plane(dx, dy),
            )
            copy.start()
            sent.append(copy)
        fwd.append(sent)
        rows_in[mine, lo:hi] = rows_out[mine, lo:hi]

    slots = X * Y * cap
    bucket = lax.broadcasted_iota(jnp.int32, (slots, tok), 0) // cap
    bucket_first = (zh * ZL + (bucket % Y) * 2 + c) * span
    bucket_slot = (bucket // Y) * 2 + zl // 4
    for m in range(ZL):
        ids = jnp.broadcast_to(ids_all[x * ZL + (2 * y + m) % ZL], (slots, tok))
        hit, _ = choose(ids, bucket_first, span, bucket_slot, cap)
        hit = jnp.where(hit, 1.0, 0.0)
        if m < 2:
            pick[m] = hit.astype(BF)
        scatter[m] = hit.T.astype(BF)

    def merge(p):
        lo, hi = cuts[p]
        for copy in fwd[p]:
            copy.wait_recv()
        for side in range(2):
            for b in range(lo, hi):
                part[side, b] = jnp.dot(
                    scatter[(side + b) % ZL],
                    rows_in[:, b, side].reshape(slots, LANE),
                    preferred_element_type=F32,
                ).astype(BF)
        copy = remote(
            part.at[1 - c, pl.ds(lo, hi - lo)], halves.at[pl.ds(lo, hi - lo)],
            half_sem.at[0, p], half_sem.at[1, p], twin,
        )
        copy.start()
        return copy

    z_copies = []
    my_block = (zl - k + ZL) % ZL
    has_block = my_block < blocks
    for d in z_offs:
        block = (z + d - k + Z) % ZL
        copy = remote(
            sums.at[jnp.minimum(block, blocks - 1)], zin.at[z],
            z_sem.at[0, d], z_sem.at[1, d], at_z(d),
        )
        z_copies.append((block, copy))

    def send_z(p, copy):
        lo, hi = cuts[p]
        copy.wait_recv()
        for b in range(lo, hi):
            sums[b] = part[c, b] + halves[b]
        for block, z_copy in z_copies:
            @pl.when((block >= lo) & (block < hi))
            def _(z_copy=z_copy):
                z_copy.start()

    twin0 = merge(0)

    twin_copies = []
    for n in range(4):
        h, m = n // 2, n % 2
        rows = pl.ds(pl.multiple_of((h * 2 + c) * feat, 16), feat)

        @pl.when(jnp.logical_not(from_self[n]))
        def _(n=n, rows=rows, m=m):
            remote(
                raw_out, raw.at[m, rows], raw_sem.at[0, 0], raw_sem.at[1, n], twin
            ).wait_recv()
        copy = remote(
            raw.at[m, rows], raw.at[m, rows], twin_sem.at[0, n], twin_sem.at[1, n], twin
        )
        copy.start()
        twin_copies.append(copy)

    send_z(0, twin0)
    for copy in twin_copies:
        copy.wait_recv()
    for m in range(2):
        got = lax.dot_general(
            pick[m], raw[m], (((1,), (1,)), ((), ())), preferred_element_type=F32
        ).astype(BF)
        back_out[:, m] = got.reshape(X * Y, cap, width)
    bwd = []
    for n, (dx, dy) in enumerate(plane_offs):
        to = ((x + dx) % X) * Y + (y + dy) % Y
        copy = remote(
            back_out.at[to], back_ref.at[mine], bwd_sem.at[0, n], bwd_sem.at[1, n],
            at_plane(dx, dy),
        )
        copy.start()
        bwd.append(copy)
    back_ref[mine] = back_out[mine]

    twin1 = merge(1)
    send_z(1, twin1)

    def columns(block, q):
        return pl.ds(pl.multiple_of(q * width + block * LANE, LANE), LANE)

    @pl.when(has_block)
    def _():
        zin[z] = sums[my_block]
        for _, copy in z_copies:
            copy.wait_recv()

    ag = []
    for q in range(4):
        cols = columns(jnp.minimum(my_block, blocks - 1), q)
        for dy in range(Y):
            if dy == 0:
                peer, sem = twin, rel_sem
            else:
                peer, sem = at_plane(0, dy), ag_sem
            ag.append(remote(
                emb_ref.at[:, cols], emb_ref.at[:, cols],
                sem.at[0, dy, q], sem.at[1, dy, q], peer,
            ))

    @pl.when(has_block)
    def _():
        for q in range(4):
            cols = columns(my_block, q)
            emb_ref[:, cols] = (zin[q] + zin[q + 4]) + (zin[q + 8] + zin[q + 12])
            for dy in (2, 1, 3, 0):
                ag[q * Y + dy].start()

    relays = []
    for dy in (1, 3, 2):
        from_k = 2 * ((y - dy + Y) % Y) + c
        from_block = (zl - from_k + ZL) % ZL
        for q in range(4):
            cols = columns(jnp.minimum(from_block, blocks - 1), q)
            relay = remote(
                emb_ref.at[:, cols], emb_ref.at[:, cols],
                rel_sem.at[0, dy, q], rel_sem.at[1, dy, q], twin,
            )
            relays.append((from_block, relay))

            @pl.when(from_block < blocks)
            def _(relay=relay, copy=ag[q * Y + dy]):
                copy.wait_recv()
                relay.start()

    for copy in bwd:
        copy.wait_recv()

    for dy in range(Y):
        other_k = 2 * ((y - dy + Y) % Y) + 1 - c
        other_block = (zl - other_k + ZL) % ZL

        @pl.when(other_block < blocks)
        def _(dy=dy):
            for q in range(4):
                remote(
                    emb_ref.at[:, columns(0, q)], emb_ref.at[:, columns(0, q)],
                    rel_sem.at[0, dy, q], rel_sem.at[1, dy, q], twin,
                ).wait_recv()

    for copies in [ids_copies, twin_copies, bwd, [twin0, twin1]] + fwd:
        for copy in copies:
            copy.wait_send()
    for a in range(4):
        @pl.when(jnp.logical_not(raw_self[a]))
        def _(a=a):
            raw_copies[a].wait_send()
    for block, copy in z_copies:
        @pl.when(block < blocks)
        def _(copy=copy):
            copy.wait_send()

    @pl.when(has_block)
    def _():
        for copy in ag:
            copy.wait_send()
    for from_block, relay in relays:
        @pl.when(from_block < blocks)
        def _(relay=relay):
            relay.wait_send()


def body(token_ids, table, out_grad, groups, segs):
    lines, width = table.shape
    tok, piece = out_grad.shape
    depth = segs * piece
    cap = tok // PACK
    blocks = width // LANE
    vmem = pl.BlockSpec(memory_space=pltpu.VMEM)
    hbm = pl.BlockSpec(memory_space=pltpu.HBM)
    dma = pltpu.SemaphoreType.DMA
    emb, back, hot = pl.pallas_call(
        kernel,
        out_shape=(
            jax.ShapeDtypeStruct((tok, depth), BF),
            jax.ShapeDtypeStruct((X * Y, 2, cap, width), BF),
            jax.ShapeDtypeStruct((groups * cap, lines), BF),
        ),
        in_specs=[vmem, hbm, hbm],
        out_specs=(vmem, vmem, vmem),
        scratch_shapes=[
            pltpu.VMEM((groups, 1, tok), jnp.int32),
            pltpu.VMEM((groups, cap, tok), jnp.int32),
            pltpu.VMEM((lines, width), BF),
            pltpu.VMEM((tok, piece), BF),
            pltpu.VMEM((piece, tok), BF),
            pltpu.VMEM((2, width, tok), BF),
            pltpu.VMEM((X * Y, blocks, 2, cap, LANE), BF),
            pltpu.VMEM((X * Y, blocks, 2, cap, LANE), BF),
            pltpu.VMEM((2, X * Y * cap, tok), BF),
            pltpu.VMEM((ZL, tok, X * Y * cap), BF),
            pltpu.VMEM((2, blocks, tok, LANE), BF),
            pltpu.VMEM((blocks, tok, LANE), BF),
            pltpu.VMEM((blocks, tok, LANE), BF),
            pltpu.VMEM((Z, tok, LANE), BF),
            pltpu.VMEM((X * Y, 2, cap, width), BF),
            dma((2,)),
            dma((2, groups)),
            dma((2, 4)),
            dma((2, 4)),
            dma((2, X * Y, 2)),
            dma((2, 2)),
            dma((2, Z)),
            dma((2, X * Y)),
            dma((2, Y, 4)),
            dma((2, Y, 4)),
        ],
        compiler_params=pltpu.CompilerParams(
            collective_id=0, has_side_effects=True, vmem_limit_bytes=48 << 20
        ),
    )(token_ids[None, :], table, out_grad)
    grad = lax.dot_general(
        hot, back.reshape(groups * cap, width), (((0,), (0,)), ((), ())),
        preferred_element_type=F32,
    )
    return emb, grad.astype(BF)


def solution(mesh):
    placed = (P("dp"), P("segment", "dp"), P("dp", "segment"))
    return jax.shard_map(
        functools.partial(body, groups=mesh.shape["dp"], segs=mesh.shape["segment"]),
        mesh=mesh,
        in_specs=placed,
        out_specs=(P("dp", None), P("segment", "dp")),
        check_vma=False,
    )
```

```python
import functools

import jax
import jax.numpy as jnp
from jax import lax
from jax.experimental import pallas as pl
from jax.experimental.pallas import tpu as pltpu
from jax.sharding import PartitionSpec as P

PACK = 8
BF = jnp.bfloat16
F32 = jnp.float32
MESH = pl.DeviceIdType.MESH

X, Y, Z, ZL = 4, 4, 16, 8
LANE = 128


def place(x, y, z, c):
    return {"segment": (z // ZL) * ZL + y * 2 + c, "dp": x * ZL + z % ZL}


def remote(src, dst, send, recv, peer):
    return pltpu.make_async_remote_copy(
        src_ref=src, dst_ref=dst, send_sem=send, recv_sem=recv,
        device_id=peer, device_id_type=MESH,
    )


def signal(sem, peer):
    pl.semaphore_signal(sem, inc=1, device_id=peer, device_id_type=MESH)


def ring(d, n):
    return min(d % n, n - d % n)


def choose(ids, first, span, slot, cap):
    rows, tok = ids.shape
    local = ids - first
    owned = (local >= 0) & (local < span) & ((ids & (PACK - 1)) == slot)
    before = lax.broadcasted_iota(jnp.int32, (tok, tok), 0) < lax.broadcasted_iota(
        jnp.int32, (tok, tok), 1
    )
    rank = jnp.dot(
        jnp.where(owned, 1.0, 0.0).astype(BF),
        jnp.where(before, 1.0, 0.0).astype(BF),
        preferred_element_type=F32,
    )
    want = lax.broadcasted_iota(jnp.int32, (rows, tok), 0) % cap
    return owned & (rank.astype(jnp.int32) == want), local


def kernel(
    ids_ref, table_ref, grad_ref,
    emb_ref, out_ref,
    ids_all, ids_wide, table, raw_out, raw_row, raw, rows_out, rows_in, pick, scatter,
    part, halves, sums, inbox, outbox, zin, back_out, back, hot,
    load_sem, ids_sem, row_sem, raw_sem, twin_sem, fwd_sem, half_sem, near_sem, z_sem, bwd_sem,
    ag_sem, rel_sem,
):
    seg = lax.axis_index("segment")
    dp = lax.axis_index("dp")
    c = seg % 2
    y = (seg // 2) % Y
    zh = seg // ZL
    zl = dp % ZL
    z = zh * ZL + zl
    x = dp // ZL
    mine = x * Y + y
    k = 2 * y + c
    lines, width = table.shape
    tok = ids_ref.shape[1]
    feat = raw_out.shape[0]
    groups = X * ZL
    cap = rows_in.shape[3]
    blocks = width // LANE
    span = lines * PACK
    twin = place(x, y, z, 1 - c)

    ids_offs = sorted(
        [(dx, dz) for dx in range(X) for dz in range(-4, 4) if (dx, dz) != (0, 0)],
        key=lambda d: -(ring(d[0], X) + abs(d[1])),
    )
    plane_offs = sorted(
        [(dx, dy) for dx in range(X) for dy in range(Y) if (dx, dy) != (0, 0)],
        key=lambda d: -(ring(d[0], X) + ring(d[1], Y)),
    )

    turn = 1 - 2 * c

    def along(d):
        return (z + turn * d + 2 * Z) % Z

    def at_z(d):
        return place(x, y, along(d), c)

    def at_ids(dx, dz):
        return place((x + dx + X) % X, y, (z + dz + Z) % Z, c)

    def at_plane(dx, dy):
        return place((x + dx + X) % X, (y + dy + Y) % Y, z, c)

    raw_to = [4 * ((y - zl // 2 - 2 * u + 8) % 4) + 2 * zh + u for u in range(2)]
    pair = (y - z // 4 - 2 * (z % 2) + 8) % 4
    raw_from = [(z % 4) // 2 * ZL + 2 * pair + m for m in range(2)]

    load_grad = pltpu.make_async_copy(grad_ref, raw_out, load_sem.at[0])
    load_grad.start()
    load = pltpu.make_async_copy(table_ref, table, load_sem.at[1])
    load.start()

    barrier = pltpu.get_barrier_semaphore()
    signal(barrier, twin)
    signal(barrier, at_ids(0, -4))
    for dx, dz in ids_offs:
        signal(barrier, at_ids(-dx, -dz))
    for dx, dy in plane_offs:
        signal(barrier, at_plane(-dx, -dy))
    for m in range(2):
        @pl.when(raw_from[m] != z)
        def _(m=m):
            signal(barrier, place(x, y, raw_from[m], c))
    n_raw = sum(jnp.where(raw_to[u] != z, 1, 0) for u in range(2))

    ids_all[dp] = ids_ref[...]
    pl.semaphore_wait(
        barrier, 2 + len(ids_offs) + len(plane_offs) + n_raw
    )

    ids_copies = []
    for n, (dx, dz) in enumerate(ids_offs):
        copy = remote(
            ids_ref, ids_all.at[dp], ids_sem.at[0, n], ids_sem.at[1, n], at_ids(dx, dz)
        )
        copy.start()
        ids_copies.append(copy)

    load_grad.wait()
    rows_sent = []
    for dy in (2, 1, 3):
        copy = remote(
            raw_out, raw_row.at[y], row_sem.at[0, dy], row_sem.at[1, dy], at_plane(0, dy)
        )
        copy.start()
        rows_sent.append(copy)
    raw_row[y] = raw_out[...]

    for copy in ids_copies:
        copy.wait_recv()

    for copy in rows_sent:
        copy.wait_recv()
    raw_copies = []
    for u in range(2):
        for v in range(2):
            rows = pl.ds(pl.multiple_of((v * 2 + c) * feat, 16), feat)
            copy = remote(
                raw_row.at[2 * u + v], raw.at[zl % 2, rows],
                raw_sem.at[0, 2 * u + v], raw_sem.at[1, v * 2 + zl % 2],
                place(x, y, raw_to[u], c),
            )
            raw_copies.append((u, copy))

            @pl.when(raw_to[u] != z)
            def _(copy=copy):
                copy.start()

            @pl.when(raw_to[u] == z)
            def _(u=u, v=v, rows=rows):
                raw[zl % 2, rows] = raw_row[2 * u + v]

    for g in range(groups):
        ids_wide[g] = jnp.broadcast_to(ids_all[g], (cap, tok))
    named, local = choose(
        ids_wide[...].reshape(groups * cap, tok), seg * span, span, dp // (groups // PACK), cap
    )
    line = jnp.sum(
        jnp.where(named, (local // PACK + 1).astype(F32), 0.0), axis=1, keepdims=True
    ).astype(jnp.int32) - 1
    hot[...] = jnp.where(
        lax.broadcasted_iota(jnp.int32, (groups * cap, lines), 1) == line, 1.0, 0.0
    ).astype(BF)
    load.wait()

    cuts = [(0, 4), (4, blocks)]
    fwd = []
    for p, (lo, hi) in enumerate(cuts):
        got = jnp.dot(
            hot[...], table[:, lo * LANE:hi * LANE], preferred_element_type=F32
        ).astype(BF)
        for g in range(groups):
            gx, j = g // ZL, g % ZL
            for b in range(lo, hi):
                core = (j - b) % ZL
                rows_out[gx * Y + core // 2, b, core % 2] = got[
                    g * cap:(g + 1) * cap, (b - lo) * LANE:(b - lo + 1) * LANE
                ]
        sent = []
        for n, (dx, dy) in enumerate(plane_offs):
            to = ((x + dx) % X) * Y + (y + dy) % Y
            copy = remote(
                rows_out.at[to, pl.ds(lo, hi - lo)], rows_in.at[mine, pl.ds(lo, hi - lo)],
                fwd_sem.at[0, n, p], fwd_sem.at[1, n, p], at_plane(dx, dy),
            )
            copy.start()
            sent.append(copy)
        fwd.append(sent)
        rows_in[mine, lo:hi] = rows_out[mine, lo:hi]

    slots = X * Y * cap
    bucket = lax.broadcasted_iota(jnp.int32, (slots, tok), 0) // cap
    bucket_first = (zh * ZL + (bucket % Y) * 2 + c) * span
    bucket_slot = (bucket // Y) * 2 + zl // 4
    for m in range(ZL):
        ids = jnp.broadcast_to(ids_all[x * ZL + m], (slots, tok))
        hit, _ = choose(ids, bucket_first, span, bucket_slot, cap)
        hit = jnp.where(hit, 1.0, 0.0)
        pick[m] = hit.astype(BF)
        scatter[m] = hit.T.astype(BF)

    def merge(p):
        lo, hi = cuts[p]
        for copy in fwd[p]:
            copy.wait_recv()
        for side in range(2):
            for b in range(lo, hi):
                part[side, b] = jnp.dot(
                    scatter[(2 * y + side + b) % ZL],
                    rows_in[:, b, side].reshape(slots, LANE),
                    preferred_element_type=F32,
                ).astype(BF)
        copy = remote(
            part.at[1 - c, pl.ds(lo, hi - lo)], halves.at[pl.ds(lo, hi - lo)],
            half_sem.at[0, p], half_sem.at[1, p], twin,
        )
        copy.start()
        return copy

    def block_of(d):
        return (along(d) - k + Z) % ZL

    def within(block, p):
        return (block >= cuts[p][0]) & (block < cuts[p][1])

    my_block = block_of(0)
    has_block = my_block < blocks
    steps = [(0, d) for d in range(4)] + [(1, -d) for d in range(1, 5)]
    near = []
    for n, (way, d) in enumerate(steps):
        block = block_of(d + (-4 if way else 4))
        near.append((block, remote(
            sums.at[jnp.minimum(block, blocks - 1)], inbox.at[n],
            near_sem.at[0, n], near_sem.at[1, n], at_z(-4 if way else 4),
        )))
    z_copies = []
    for n, (way, d) in enumerate(steps):
        z_copies.append((block_of(d), None if d == 0 else remote(
            outbox.at[n], zin.at[way, z % 4], z_sem.at[0, n], z_sem.at[1, n], at_z(d),
        )))
    order = sorted(range(8), key=lambda n: -abs(steps[n][1]))

    def send_z(p, copy):
        lo, hi = cuts[p]
        copy.wait_recv()
        for b in range(lo, hi):
            sums[b] = part[c, b] + halves[b]
        for n in order:
            block, near_copy = near[n]

            @pl.when(within(block, p))
            def _(near_copy=near_copy):
                near_copy.start()

    def pass_z(p):
        for n in order:
            block, z_copy = z_copies[n]

            @pl.when(within(block, p))
            def _(n=n, block=block, z_copy=z_copy):
                near[n][1].wait_recv()
                both = sums[block] + inbox[n]
                if steps[n][1] == 0:
                    zin[0, z % 4] = both
                else:
                    outbox[n] = both
                    z_copy.start()

    twin0 = merge(0)

    send_z(0, twin0)
    twin1 = merge(1)
    send_z(1, twin1)

    twin_copies = []
    for n in range(4):
        v, m = n // 2, n % 2
        rows = pl.ds(pl.multiple_of((v * 2 + c) * feat, 16), feat)
        copy = remote(
            raw.at[m, rows], raw.at[m, rows], twin_sem.at[0, n], twin_sem.at[1, n], twin
        )

        @pl.when(raw_from[m] != z)
        def _(n=n, m=m, rows=rows):
            remote(
                raw_out, raw.at[m, rows], raw_sem.at[0, 0], raw_sem.at[1, n], twin
            ).wait_recv()
        copy.start()
        twin_copies.append(copy)

    for copy in twin_copies:
        copy.wait_recv()
    for m in range(2):
        got = lax.dot_general(
            pick[2 * pair + m], raw[m], (((1,), (1,)), ((), ())), preferred_element_type=F32
        ).astype(BF)
        back_out[:, m] = got.reshape(X * Y, cap, width)
    bwd = []
    for n, (dx, dy) in enumerate(plane_offs):
        to = ((x + dx) % X) * Y + (y + dy) % Y
        copy = remote(
            back_out.at[to], back.at[x * Y + pair], bwd_sem.at[0, n], bwd_sem.at[1, n],
            at_plane(dx, dy),
        )
        copy.start()
        bwd.append(copy)
    back[x * Y + pair] = back_out[mine]

    pass_z(0)
    pass_z(1)

    def columns(block, q):
        return pl.ds(pl.multiple_of(q * width + block * LANE, LANE), LANE)

    def quarter(d):
        return (along(-d)) % 4

    ag = []
    for d in range(4):
        cols = columns(jnp.minimum(my_block, blocks - 1), quarter(d))
        for dy in range(Y):
            if dy == 0:
                peer, sem = twin, rel_sem
            else:
                peer, sem = at_plane(0, dy), ag_sem
            ag.append(remote(
                emb_ref.at[:, cols], emb_ref.at[:, cols],
                sem.at[0, dy, d], sem.at[1, dy, d], peer,
            ))

    @pl.when(has_block)
    def _():
        for d in range(4):
            if d > 0:
                z_copies[d][1].wait_recv()
            z_copies[3 + 4 - d][1].wait_recv()
            cols = columns(my_block, quarter(d))
            emb_ref[:, cols] = zin[0, quarter(d)] + zin[1, quarter(d)]
            for dy in (2, 1, 3, 0):
                ag[d * Y + dy].start()

    for copy in bwd:
        copy.wait_recv()
    out_ref[...] = lax.dot_general(
        hot[...], back[...].reshape(groups * cap, width), (((0,), (0,)), ((), ())),
        preferred_element_type=F32,
    ).astype(BF)

    relays = []
    for dy in (1, 3, 2):
        from_k = 2 * ((y - dy + Y) % Y) + c
        from_block = (zl - from_k + ZL) % ZL
        for q in range(4):
            cols = columns(jnp.minimum(from_block, blocks - 1), quarter(q))
            relay = remote(
                emb_ref.at[:, cols], emb_ref.at[:, cols],
                rel_sem.at[0, dy, q], rel_sem.at[1, dy, q], twin,
            )
            relays.append((from_block, relay))

            @pl.when(from_block < blocks)
            def _(relay=relay, copy=ag[q * Y + dy]):
                copy.wait_recv()
                relay.start()

    for dy in range(Y):
        other_k = 2 * ((y - dy + Y) % Y) + 1 - c
        other_block = (zl - other_k + ZL) % ZL

        @pl.when(other_block < blocks)
        def _(dy=dy):
            for q in range(4):
                remote(
                    emb_ref.at[:, columns(0, q)], emb_ref.at[:, columns(0, q)],
                    rel_sem.at[0, dy, q], rel_sem.at[1, dy, q], twin,
                ).wait_recv()

    for copies in [ids_copies, rows_sent, twin_copies, bwd, [twin0, twin1]] + fwd:
        for copy in copies:
            copy.wait_send()
    for u, copy in raw_copies:
        @pl.when(raw_to[u] != z)
        def _(copy=copy):
            copy.wait_send()
    for block, copy in near:
        @pl.when(block < blocks)
        def _(copy=copy):
            copy.wait_send()
    for block, copy in z_copies[1:]:
        @pl.when(block < blocks)
        def _(copy=copy):
            copy.wait_send()

    @pl.when(has_block)
    def _():
        for copy in ag:
            copy.wait_send()
    for from_block, relay in relays:
        @pl.when(from_block < blocks)
        def _(relay=relay):
            relay.wait_send()


def body(token_ids, table, out_grad, groups, segs):
    lines, width = table.shape
    tok, piece = out_grad.shape
    depth = segs * piece
    cap = tok // PACK
    blocks = width // LANE
    vmem = pl.BlockSpec(memory_space=pltpu.VMEM)
    hbm = pl.BlockSpec(memory_space=pltpu.HBM)
    dma = pltpu.SemaphoreType.DMA
    return pl.pallas_call(
        kernel,
        out_shape=(
            jax.ShapeDtypeStruct((tok, depth), BF),
            jax.ShapeDtypeStruct((lines, width), BF),
        ),
        in_specs=[vmem, hbm, hbm],
        out_specs=(vmem, vmem),
        scratch_shapes=[
            pltpu.VMEM((groups, 1, tok), jnp.int32),
            pltpu.VMEM((groups, cap, tok), jnp.int32),
            pltpu.VMEM((lines, width), BF),
            pltpu.VMEM((piece, tok), BF),
            pltpu.VMEM((Y, piece, tok), BF),
            pltpu.VMEM((2, width, tok), BF),
            pltpu.VMEM((X * Y, blocks, 2, cap, LANE), BF),
            pltpu.VMEM((X * Y, blocks, 2, cap, LANE), BF),
            pltpu.VMEM((ZL, X * Y * cap, tok), BF),
            pltpu.VMEM((ZL, tok, X * Y * cap), BF),
            pltpu.VMEM((2, blocks, tok, LANE), BF),
            pltpu.VMEM((blocks, tok, LANE), BF),
            pltpu.VMEM((blocks, tok, LANE), BF),
            pltpu.VMEM((8, tok, LANE), BF),
            pltpu.VMEM((8, tok, LANE), BF),
            pltpu.VMEM((2, 4, tok, LANE), BF),
            pltpu.VMEM((X * Y, 2, cap, width), BF),
            pltpu.VMEM((X * Y, 2, cap, width), BF),
            pltpu.VMEM((groups * cap, lines), BF),
            dma((2,)),
            dma((2, groups)),
            dma((2, Y)),
            dma((2, 4)),
            dma((2, 4)),
            dma((2, X * Y, 2)),
            dma((2, 2)),
            dma((2, 8)),
            dma((2, 8)),
            dma((2, X * Y)),
            dma((2, Y, 4)),
            dma((2, Y, 4)),
        ],
        compiler_params=pltpu.CompilerParams(
            collective_id=0, has_side_effects=True, vmem_limit_bytes=50 << 20
        ),
    )(token_ids[None, :], table, out_grad.T)


def solution(mesh):
    placed = (P("dp"), P("segment", "dp"), P("dp", "segment"))
    return jax.shard_map(
        functools.partial(body, groups=mesh.shape["dp"], segs=mesh.shape["segment"]),
        mesh=mesh,
        in_specs=placed,
        out_specs=(P("dp", None), P("segment", "dp")),
        check_vma=False,
    )
```

```python
import functools

import jax
import jax.numpy as jnp
from jax import lax
from jax.experimental import pallas as pl
from jax.experimental.pallas import tpu as pltpu
from jax.sharding import PartitionSpec as P

PACK = 8
BF = jnp.bfloat16
F32 = jnp.float32
MESH = pl.DeviceIdType.MESH

X, Y, Z, ZL = 4, 4, 16, 8
LANE = 128


def place(x, y, z, c):
    return {"segment": (z // ZL) * ZL + y * 2 + c, "dp": x * ZL + z % ZL}


def remote(src, dst, send, recv, peer):
    return pltpu.make_async_remote_copy(
        src_ref=src, dst_ref=dst, send_sem=send, recv_sem=recv,
        device_id=peer, device_id_type=MESH,
    )


def arrived(ref, sem, peer):
    remote(ref, ref, sem, sem, peer).wait_recv()


def left(ref, sem, peer):
    remote(ref, ref, sem, sem, peer).wait_send()


def signal(sem, peer):
    pl.semaphore_signal(sem, inc=1, device_id=peer, device_id_type=MESH)


def ring(d, n):
    return min(d % n, n - d % n)


def choose(ids, first, span, slot, cap):
    rows, tok = ids.shape
    local = ids - first
    owned = (local >= 0) & (local < span) & ((ids & (PACK - 1)) == slot)
    before = lax.broadcasted_iota(jnp.int32, (tok, tok), 0) < lax.broadcasted_iota(
        jnp.int32, (tok, tok), 1
    )
    rank = jnp.dot(
        jnp.where(owned, 1.0, 0.0).astype(BF),
        jnp.where(before, 1.0, 0.0).astype(BF),
        preferred_element_type=F32,
    )
    want = lax.broadcasted_iota(jnp.int32, (rows, tok), 0) % cap
    return owned & (rank.astype(jnp.int32) == want), local


def kernel(
    ids_hbm, table_ref, grad_ref,
    emb_ref, out_ref,
    ids_ref, ids_all, ids_wide, table, raw_out, raw_row, raw, rows_out, rows_in, pick, scatter,
    part, halves, sums, inbox, outbox, zin, back_out, back, hot,
    load_sem, ids_sem, row_sem, raw_sem, twin_sem, fwd_sem, half_sem, near_sem, z_sem, bwd_sem,
    ag_sem, rel_sem,
):
    seg = lax.axis_index("segment")
    dp = lax.axis_index("dp")
    c = seg % 2
    y = (seg // 2) % Y
    zh = seg // ZL
    zl = dp % ZL
    z = zh * ZL + zl
    x = dp // ZL
    mine = x * Y + y
    k = 2 * y + c
    lines, width = table.shape
    tok = ids_ref.shape[1]
    feat = raw_out.shape[0]
    groups = X * ZL
    cap = rows_in.shape[3]
    blocks = width // LANE
    span = lines * PACK
    twin = place(x, y, z, 1 - c)

    ids_offs = sorted(
        [(dx, dz) for dx in range(X) for dz in range(-4, 4) if (dx, dz) != (0, 0)],
        key=lambda d: -(ring(d[0], X) + abs(d[1])),
    )
    plane_offs = sorted(
        [(dx, dy) for dx in range(X) for dy in range(Y) if (dx, dy) != (0, 0)],
        key=lambda d: -(ring(d[0], X) + ring(d[1], Y)),
    )

    turn = 1 - 2 * c

    def along(d):
        return (z + turn * d + 2 * Z) % Z

    def at_z(d):
        return place(x, y, along(d), c)

    def at_ids(dx, dz):
        return place((x + dx + X) % X, y, (z + dz + Z) % Z, c)

    def at_plane(dx, dy):
        return place((x + dx + X) % X, (y + dy + Y) % Y, z, c)

    raw_to = [4 * ((y - zl // 2 - 2 * u + 8) % 4) + 2 * zh + u for u in range(2)]
    pair = (y - z // 4 - 2 * (z % 2) + 8) % 4
    raw_from = [(z % 4) // 2 * ZL + 2 * pair + m for m in range(2)]

    load_ids = pltpu.make_async_copy(ids_hbm, ids_ref, load_sem.at[2])
    load_ids.start()
    load_grad = pltpu.make_async_copy(grad_ref, raw_out, load_sem.at[0])
    load_grad.start()
    load = pltpu.make_async_copy(table_ref, table, load_sem.at[1])
    load.start()

    barrier = pltpu.get_barrier_semaphore()
    signal(barrier, twin)
    signal(barrier, at_ids(0, -4))
    for dx, dz in ids_offs:
        signal(barrier, at_ids(-dx, -dz))
    for dx, dy in plane_offs:
        signal(barrier, at_plane(-dx, -dy))
    for m in range(2):
        @pl.when(raw_from[m] != z)
        def _(m=m):
            signal(barrier, place(x, y, raw_from[m], c))
    n_raw = sum(jnp.where(raw_to[u] != z, 1, 0) for u in range(2))

    load_ids.wait()
    ids_all[dp] = ids_ref[...]
    pl.semaphore_wait(
        barrier, 2 + len(ids_offs) + len(plane_offs) + n_raw
    )

    for dx, dz in ids_offs:
        remote(
            ids_ref, ids_all.at[dp], ids_sem.at[0], ids_sem.at[1], at_ids(dx, dz)
        ).start()

    load_grad.wait()
    for dy in (2, 1, 3):
        remote(
            raw_out, raw_row.at[y], row_sem.at[0], row_sem.at[1], at_plane(0, dy)
        ).start()
    raw_row[y] = raw_out[...]

    arrived(raw_row.at[pl.ds(0, Y - 1)], row_sem.at[1], twin)
    for u in range(2):
        for v in range(2):
            rows = pl.ds(pl.multiple_of((v * 2 + c) * feat, 16), feat)
            copy = remote(
                raw_row.at[2 * u + v], raw.at[zl % 2, rows],
                raw_sem.at[0, u], raw_sem.at[1, zl % 2],
                place(x, y, raw_to[u], c),
            )

            @pl.when(raw_to[u] != z)
            def _(copy=copy):
                copy.start()

            @pl.when(raw_to[u] == z)
            def _(u=u, v=v, rows=rows):
                raw[zl % 2, rows] = raw_row[2 * u + v]

    arrived(ids_all.at[pl.ds(0, groups - 1)], ids_sem.at[1], twin)

    for g in range(groups):
        ids_wide[g] = jnp.broadcast_to(ids_all[g], (cap, tok))
    named, local = choose(
        ids_wide[...].reshape(groups * cap, tok), seg * span, span, dp // (groups // PACK), cap
    )
    line = jnp.sum(
        jnp.where(named, (local // PACK + 1).astype(F32), 0.0), axis=1, keepdims=True
    ).astype(jnp.int32) - 1
    hot[...] = jnp.where(
        lax.broadcasted_iota(jnp.int32, (groups * cap, lines), 1) == line, 1.0, 0.0
    ).astype(BF)
    load.wait()

    cuts = [(0, 4), (4, blocks)]
    for p, (lo, hi) in enumerate(cuts):
        got = jnp.dot(
            hot[...], table[:, lo * LANE:hi * LANE], preferred_element_type=F32
        ).astype(BF)
        for g in range(groups):
            gx, j = g // ZL, g % ZL
            for b in range(lo, hi):
                core = (j - b) % ZL
                rows_out[gx * Y + core // 2, b, core % 2] = got[
                    g * cap:(g + 1) * cap, (b - lo) * LANE:(b - lo + 1) * LANE
                ]
        for dx, dy in plane_offs:
            to = ((x + dx) % X) * Y + (y + dy) % Y
            remote(
                rows_out.at[to, pl.ds(lo, hi - lo)], rows_in.at[mine, pl.ds(lo, hi - lo)],
                fwd_sem.at[0, p], fwd_sem.at[1, p], at_plane(dx, dy),
            ).start()
        rows_in[mine, lo:hi] = rows_out[mine, lo:hi]

    slots = X * Y * cap
    bucket = lax.broadcasted_iota(jnp.int32, (slots, tok), 0) // cap
    bucket_first = (zh * ZL + (bucket % Y) * 2 + c) * span
    bucket_slot = (bucket // Y) * 2 + zl // 4
    for m in range(ZL):
        ids = jnp.broadcast_to(ids_all[x * ZL + m], (slots, tok))
        hit, _ = choose(ids, bucket_first, span, bucket_slot, cap)
        hit = jnp.where(hit, 1.0, 0.0)
        pick[m] = hit.astype(BF)
        scatter[m] = hit.T.astype(BF)

    def merge(p):
        lo, hi = cuts[p]
        arrived(rows_in.at[pl.ds(0, X * Y - 1), pl.ds(lo, hi - lo)], fwd_sem.at[1, p], twin)
        for side in range(2):
            for b in range(lo, hi):
                part[side, b] = jnp.dot(
                    scatter[(2 * y + side + b) % ZL],
                    rows_in[:, b, side].reshape(slots, LANE),
                    preferred_element_type=F32,
                ).astype(BF)
        copy = remote(
            part.at[1 - c, pl.ds(lo, hi - lo)], halves.at[pl.ds(lo, hi - lo)],
            half_sem.at[0, p], half_sem.at[1, p], twin,
        )
        copy.start()
        return copy

    def block_of(d):
        return (along(d) - k + Z) % ZL

    def within(block, p):
        return (block >= cuts[p][0]) & (block < cuts[p][1])

    my_block = block_of(0)
    has_block = my_block < blocks
    steps = [(0, d) for d in range(4)] + [(1, -d) for d in range(1, 5)]
    near = []
    for n, (way, d) in enumerate(steps):
        block = block_of(d + (-4 if way else 4))
        near.append((block, remote(
            sums.at[jnp.minimum(block, blocks - 1)], inbox.at[n],
            near_sem.at[8], near_sem.at[n], at_z(-4 if way else 4),
        )))
    z_copies = []
    for n, (way, d) in enumerate(steps):
        z_copies.append((block_of(d), None if d == 0 else remote(
            outbox.at[n], zin.at[way, z % 4], z_sem.at[4], z_sem.at[d % 4], at_z(d),
        )))
    order = sorted(range(8), key=lambda n: -abs(steps[n][1]))

    def send_z(p, copy):
        lo, hi = cuts[p]
        copy.wait_recv()
        for b in range(lo, hi):
            sums[b] = part[c, b] + halves[b]
        for n in order:
            block, near_copy = near[n]

            @pl.when(within(block, p))
            def _(near_copy=near_copy):
                near_copy.start()

    def pass_z(p):
        for n in order:
            block, z_copy = z_copies[n]

            @pl.when(within(block, p))
            def _(n=n, block=block, z_copy=z_copy):
                near[n][1].wait_recv()
                both = sums[block] + inbox[n]
                if steps[n][1] == 0:
                    zin[0, z % 4] = both
                else:
                    outbox[n] = both
                    z_copy.start()

    twin0 = merge(0)

    send_z(0, twin0)
    twin1 = merge(1)
    send_z(1, twin1)

    for m in range(2):
        @pl.when(raw_from[m] != z)
        def _(m=m):
            arrived(raw_row.at[pl.ds(0, 2)], raw_sem.at[1, m], twin)
        for v in range(2):
            rows = pl.ds(pl.multiple_of((v * 2 + c) * feat, 16), feat)
            remote(
                raw.at[m, rows], raw.at[m, rows], twin_sem.at[0], twin_sem.at[1], twin
            ).start()

    arrived(raw_row, twin_sem.at[1], twin)
    for m in range(2):
        got = lax.dot_general(
            pick[2 * pair + m], raw[m], (((1,), (1,)), ((), ())), preferred_element_type=F32
        ).astype(BF)
        back_out[:, m] = got.reshape(X * Y, cap, width)
    for dx, dy in plane_offs:
        to = ((x + dx) % X) * Y + (y + dy) % Y
        remote(
            back_out.at[to], back.at[x * Y + pair], bwd_sem.at[0], bwd_sem.at[1],
            at_plane(dx, dy),
        ).start()
    back[x * Y + pair] = back_out[mine]

    pass_z(0)
    pass_z(1)

    def columns(block, q):
        return pl.ds(pl.multiple_of(q * width + block * LANE, LANE), LANE)

    def quarter(d):
        return (along(-d)) % 4

    ag = []
    for d in range(4):
        cols = columns(jnp.minimum(my_block, blocks - 1), quarter(d))
        for dy in range(Y):
            if dy == 0:
                peer, out, sem = twin, rel_sem.at[4], rel_sem
            else:
                peer, out, sem = at_plane(0, dy), ag_sem.at[0], ag_sem
            ag.append(remote(
                emb_ref.at[:, cols], emb_ref.at[:, cols],
                out, sem.at[dy], peer,
            ))

    @pl.when(has_block)
    def _():
        for d in range(4):
            arrived(outbox.at[pl.ds(0, 2 if d else 1)], z_sem.at[d], twin)
            cols = columns(my_block, quarter(d))
            emb_ref[:, cols] = zin[0, quarter(d)] + zin[1, quarter(d)]
            for dy in (2, 1, 3, 0):
                ag[d * Y + dy].start()

    arrived(back.at[pl.ds(0, X * Y - 1)], bwd_sem.at[1], twin)
    out_ref[...] = lax.dot_general(
        hot[...], back[...].reshape(groups * cap, width), (((0,), (0,)), ((), ())),
        preferred_element_type=F32,
    ).astype(BF)

    four = emb_ref.at[:, pl.ds(0, 4 * LANE)]
    for dy in (1, 3, 2):
        from_k = 2 * ((y - dy + Y) % Y) + c
        from_block = (zl - from_k + ZL) % ZL

        @pl.when(from_block < blocks)
        def _(dy=dy, from_block=from_block):
            arrived(four, ag_sem.at[dy], twin)
            for q in range(4):
                cols = columns(from_block, q)
                remote(
                    emb_ref.at[:, cols], emb_ref.at[:, cols], rel_sem.at[4], rel_sem.at[dy], twin
                ).start()

    for dy in range(Y):
        other_k = 2 * ((y - dy + Y) % Y) + 1 - c
        other_block = (zl - other_k + ZL) % ZL

        @pl.when(other_block < blocks)
        def _(dy=dy):
            arrived(four, rel_sem.at[dy], twin)

    left(ids_all.at[pl.ds(0, groups - 1)], ids_sem.at[0], twin)
    left(raw_row.at[pl.ds(0, Y - 1)], row_sem.at[0], twin)
    for u in range(2):
        @pl.when(raw_to[u] != z)
        def _(u=u):
            left(raw_row.at[pl.ds(0, 2)], raw_sem.at[0, u], twin)
    left(raw_row, twin_sem.at[0], twin)
    for p, (lo, hi) in enumerate(cuts):
        left(rows_in.at[pl.ds(0, X * Y - 1), pl.ds(lo, hi - lo)], fwd_sem.at[0, p], twin)
    twin0.wait_send()
    twin1.wait_send()
    left(back.at[pl.ds(0, X * Y - 1)], bwd_sem.at[0], twin)
    left(outbox.at[pl.ds(0, 7)], near_sem.at[8], twin)

    @pl.when(has_block)
    def _():
        left(outbox.at[pl.ds(0, 6)], z_sem.at[4], twin)
        left(emb_ref.at[:, pl.ds(0, 12 * LANE)], ag_sem.at[0], twin)

    @pl.when(jnp.logical_not(has_block))
    def _():
        left(outbox.at[pl.ds(0, 7)], z_sem.at[4], twin)

    full = (zl + 1) % 2 != c

    @pl.when(full)
    def _():
        left(emb_ref.at[:, pl.ds(0, 16 * LANE)], rel_sem.at[4], twin)

    @pl.when(jnp.logical_not(full))
    def _():
        left(emb_ref.at[:, pl.ds(0, 12 * LANE)], rel_sem.at[4], twin)


def store(emb_ref, grad_ref, emb_out, grad_out, sem):
    copies = [
        pltpu.make_async_copy(grad_ref, grad_out, sem.at[0]),
        pltpu.make_async_copy(emb_ref, emb_out, sem.at[1]),
    ]
    for copy in copies:
        copy.start()
    for copy in copies:
        copy.wait()


def body(token_ids, table, out_grad, groups, segs):
    lines, width = table.shape
    tok, piece = out_grad.shape
    depth = segs * piece
    cap = tok // PACK
    blocks = width // LANE
    vmem = pl.BlockSpec(memory_space=pltpu.VMEM)
    hbm = pl.BlockSpec(memory_space=pltpu.HBM)
    dma = pltpu.SemaphoreType.DMA
    shapes = (
        jax.ShapeDtypeStruct((tok, depth), BF),
        jax.ShapeDtypeStruct((lines, width), BF),
    )
    emb, grad = pl.pallas_call(
        kernel,
        out_shape=shapes,
        in_specs=[hbm, hbm, hbm],
        out_specs=(vmem, vmem),
        scratch_shapes=[
            pltpu.VMEM((1, tok), jnp.int32),
            pltpu.VMEM((groups, 1, tok), jnp.int32),
            pltpu.VMEM((groups, cap, tok), jnp.int32),
            pltpu.VMEM((lines, width), BF),
            pltpu.VMEM((piece, tok), BF),
            pltpu.VMEM((Y, piece, tok), BF),
            pltpu.VMEM((2, width, tok), BF),
            pltpu.VMEM((X * Y, blocks, 2, cap, LANE), BF),
            pltpu.VMEM((X * Y, blocks, 2, cap, LANE), BF),
            pltpu.VMEM((ZL, X * Y * cap, tok), BF),
            pltpu.VMEM((ZL, tok, X * Y * cap), BF),
            pltpu.VMEM((2, blocks, tok, LANE), BF),
            pltpu.VMEM((blocks, tok, LANE), BF),
            pltpu.VMEM((blocks, tok, LANE), BF),
            pltpu.VMEM((8, tok, LANE), BF),
            pltpu.VMEM((8, tok, LANE), BF),
            pltpu.VMEM((2, 4, tok, LANE), BF),
            pltpu.VMEM((X * Y, 2, cap, width), BF),
            pltpu.VMEM((X * Y, 2, cap, width), BF),
            pltpu.VMEM((groups * cap, lines), BF),
            dma((3,)),
            dma((2,)),
            dma((2,)),
            dma((2, 2)),
            dma((2,)),
            dma((2, 2)),
            dma((2, 2)),
            dma((9,)),
            dma((5,)),
            dma((2,)),
            dma((4,)),
            dma((5,)),
        ],
        compiler_params=pltpu.CompilerParams(
            collective_id=0, has_side_effects=True, vmem_limit_bytes=50 << 20
        ),
    )(*[
        pltpu.with_memory_space_constraint(a, pltpu.HBM)
        for a in (token_ids[None, :], table, out_grad.T)
    ])
    return pl.pallas_call(
        store,
        out_shape=shapes,
        in_specs=[vmem, vmem],
        out_specs=(hbm, hbm),
        scratch_shapes=[dma((2,))],
        compiler_params=pltpu.CompilerParams(vmem_limit_bytes=50 << 20),
    )(emb, grad)


def solution(mesh):
    placed = (P("dp"), P("segment", "dp"), P("dp", "segment"))
    return jax.shard_map(
        functools.partial(body, groups=mesh.shape["dp"], segs=mesh.shape["segment"]),
        mesh=mesh,
        in_specs=placed,
        out_specs=(P("dp", None), P("segment", "dp")),
        check_vma=False,
    )
```

```python
import functools

import jax
import jax.numpy as jnp
from jax import lax
from jax.experimental import pallas as pl
from jax.experimental.pallas import tpu as pltpu
from jax.sharding import PartitionSpec as P

PACK = 8
BF = jnp.bfloat16
F32 = jnp.float32
MESH = pl.DeviceIdType.MESH

X, Y, Z, ZL = 4, 4, 16, 8
LANE = 128


def place(x, y, z, c):
    return {"segment": (z // ZL) * ZL + y * 2 + c, "dp": x * ZL + z % ZL}


def remote(src, dst, send, recv, peer):
    return pltpu.make_async_remote_copy(
        src_ref=src, dst_ref=dst, send_sem=send, recv_sem=recv,
        device_id=peer, device_id_type=MESH,
    )


def arrived(ref, sem, peer):
    remote(ref, ref, sem, sem, peer).wait_recv()


def left(ref, sem, peer):
    remote(ref, ref, sem, sem, peer).wait_send()


def signal(sem, peer):
    pl.semaphore_signal(sem, inc=1, device_id=peer, device_id_type=MESH)


def ring(d, n):
    return min(d % n, n - d % n)


def choose(ids, first, span, slot, cap):
    rows, tok = ids.shape
    local = ids - first
    owned = (local >= 0) & (local < span) & ((ids & (PACK - 1)) == slot)
    before = lax.broadcasted_iota(jnp.int32, (tok, tok), 0) < lax.broadcasted_iota(
        jnp.int32, (tok, tok), 1
    )
    rank = jnp.dot(
        jnp.where(owned, 1.0, 0.0).astype(BF),
        jnp.where(before, 1.0, 0.0).astype(BF),
        preferred_element_type=F32,
    )
    want = lax.broadcasted_iota(jnp.int32, (rows, tok), 0) % cap
    return owned & (rank.astype(jnp.int32) == want), local


def kernel(
    ids_hbm, table_ref, grad_ref,
    emb_ref, out_ref,
    ids_ref, ids_all, ids_wide, table, raw_out, raw_row, raw, rows_out, rows_in, pick, scatter,
    part, halves, sums, inbox, outbox, zin, back_out, back, hot,
    load_sem, ids_sem, row_sem, raw_sem, twin_sem, fwd_sem, half_sem, near_sem, z_sem, bwd_sem,
    ag_sem, rel_sem,
):
    seg = lax.axis_index("segment")
    dp = lax.axis_index("dp")
    c = seg % 2
    y = (seg // 2) % Y
    zh = seg // ZL
    zl = dp % ZL
    z = zh * ZL + zl
    x = dp // ZL
    mine = x * Y + y
    k = 2 * y + c
    lines, width = table.shape
    tok = ids_ref.shape[1]
    feat = raw_out.shape[0]
    groups = X * ZL
    cap = rows_in.shape[3]
    blocks = width // LANE
    span = lines * PACK
    twin = place(x, y, z, 1 - c)

    ids_offs = sorted(
        [(dx, dz) for dx in range(X) for dz in range(-4, 4) if (dx, dz) != (0, 0)],
        key=lambda d: -(ring(d[0], X) + abs(d[1])),
    )
    plane_offs = sorted(
        [(dx, dy) for dx in range(X) for dy in range(Y) if (dx, dy) != (0, 0)],
        key=lambda d: -(ring(d[0], X) + ring(d[1], Y)),
    )

    turn = 1 - 2 * c

    def along(d):
        return (z + turn * d + 2 * Z) % Z

    def at_z(d):
        return place(x, y, along(d), c)

    def at_ids(dx, dz):
        return place((x + dx + X) % X, y, (z + dz + Z) % Z, c)

    def at_plane(dx, dy):
        return place((x + dx + X) % X, (y + dy + Y) % Y, z, c)

    raw_to = [4 * ((y - zl // 2 - 2 * u + 8) % 4) + 2 * zh + u for u in range(2)]
    pair = (y - z // 4 - 2 * (z % 2) + 8) % 4
    raw_from = [(z % 4) // 2 * ZL + 2 * pair + m for m in range(2)]

    load_ids = pltpu.make_async_copy(ids_hbm, ids_ref, load_sem.at[2])
    load_ids.start()
    load_grad = pltpu.make_async_copy(grad_ref, raw_out, load_sem.at[0])
    load_grad.start()
    load = pltpu.make_async_copy(table_ref, table, load_sem.at[1])
    load.start()

    barrier = pltpu.get_barrier_semaphore()
    signal(barrier, twin)
    signal(barrier, at_ids(0, -4))
    for dx, dz in ids_offs:
        signal(barrier, at_ids(-dx, -dz))
    for dx, dy in plane_offs:
        signal(barrier, at_plane(-dx, -dy))
    for m in range(2):
        @pl.when(raw_from[m] != z)
        def _(m=m):
            signal(barrier, place(x, y, raw_from[m], c))
    n_raw = sum(jnp.where(raw_to[u] != z, 1, 0) for u in range(2))

    load_ids.wait()
    ids_all[dp] = ids_ref[...]
    pl.semaphore_wait(
        barrier, 2 + len(ids_offs) + len(plane_offs) + n_raw
    )

    for dx, dz in ids_offs:
        remote(
            ids_ref, ids_all.at[dp], ids_sem.at[0], ids_sem.at[1], at_ids(dx, dz)
        ).start()

    load_grad.wait()
    for dy in (2, 1, 3):
        remote(
            raw_out, raw_row.at[y], row_sem.at[0], row_sem.at[1], at_plane(0, dy)
        ).start()
    raw_row[y] = raw_out[...]

    arrived(raw_row.at[pl.ds(0, Y - 1)], row_sem.at[1], twin)
    for u in range(2):
        for v in range(2):
            rows = pl.ds(pl.multiple_of((v * 2 + c) * feat, 16), feat)
            copy = remote(
                raw_row.at[2 * u + v], raw.at[zl % 2, rows],
                raw_sem.at[0, u], raw_sem.at[1, zl % 2],
                place(x, y, raw_to[u], c),
            )

            @pl.when(raw_to[u] != z)
            def _(copy=copy):
                copy.start()

            @pl.when(raw_to[u] == z)
            def _(u=u, v=v, rows=rows):
                raw[zl % 2, rows] = raw_row[2 * u + v]

    arrived(ids_all.at[pl.ds(0, groups - 1)], ids_sem.at[1], twin)

    for g in range(groups):
        ids_wide[g] = jnp.broadcast_to(ids_all[g], (cap, tok))
    named, local = choose(
        ids_wide[...].reshape(groups * cap, tok), seg * span, span, dp // (groups // PACK), cap
    )
    line = jnp.sum(
        jnp.where(named, (local // PACK + 1).astype(F32), 0.0), axis=1, keepdims=True
    ).astype(jnp.int32) - 1
    hot[...] = jnp.where(
        lax.broadcasted_iota(jnp.int32, (groups * cap, lines), 1) == line, 1.0, 0.0
    ).astype(BF)
    load.wait()

    cuts = [(0, 4), (4, blocks)]
    for p, (lo, hi) in enumerate(cuts):
        got = jnp.dot(
            hot[...], table[:, lo * LANE:hi * LANE], preferred_element_type=F32
        ).astype(BF)
        for g in range(groups):
            gx, j = g // ZL, g % ZL
            for b in range(lo, hi):
                core = (j - b) % ZL
                rows_out[gx * Y + core // 2, b, core % 2] = got[
                    g * cap:(g + 1) * cap, (b - lo) * LANE:(b - lo + 1) * LANE
                ]
        for dx, dy in plane_offs:
            to = ((x + dx) % X) * Y + (y + dy) % Y
            remote(
                rows_out.at[to, pl.ds(lo, hi - lo)], rows_in.at[mine, pl.ds(lo, hi - lo)],
                fwd_sem.at[0, p], fwd_sem.at[1, p], at_plane(dx, dy),
            ).start()
        rows_in[mine, lo:hi] = rows_out[mine, lo:hi]

    slots = X * Y * cap
    bucket = lax.broadcasted_iota(jnp.int32, (slots, tok), 0) // cap
    bucket_first = (zh * ZL + (bucket % Y) * 2 + c) * span
    bucket_slot = (bucket // Y) * 2 + zl // 4
    for m in range(ZL):
        ids = jnp.broadcast_to(ids_all[x * ZL + m], (slots, tok))
        hit, _ = choose(ids, bucket_first, span, bucket_slot, cap)
        hit = jnp.where(hit, 1.0, 0.0)
        pick[m] = hit.astype(BF)
        scatter[m] = hit.T.astype(BF)

    def merge(p):
        lo, hi = cuts[p]
        arrived(rows_in.at[pl.ds(0, X * Y - 1), pl.ds(lo, hi - lo)], fwd_sem.at[1, p], twin)
        for side in range(2):
            for b in range(lo, hi):
                part[side, b] = jnp.dot(
                    scatter[(2 * y + side + b) % ZL],
                    rows_in[:, b, side].reshape(slots, LANE),
                    preferred_element_type=F32,
                ).astype(BF)
        copy = remote(
            part.at[1 - c, pl.ds(lo, hi - lo)], halves.at[pl.ds(lo, hi - lo)],
            half_sem.at[0, p], half_sem.at[1, p], twin,
        )
        copy.start()
        return copy

    def block_of(d):
        return (along(d) - k + Z) % ZL

    ranks = [(0, 2), (2, Z)]

    def within(block, p, plane, r):
        return (
            (block >= cuts[p][0]) & (block < cuts[p][1])
            & (plane >= ranks[r][0]) & (plane < ranks[r][1])
        )

    my_block = block_of(0)
    has_block = my_block < blocks
    steps = [(0, d) for d in range(4)] + [(1, -d) for d in range(1, 5)]
    near = []
    for n, (way, d) in enumerate(steps):
        block = block_of(d + (-4 if way else 4))
        near.append((block, along(d + (-4 if way else 4)), remote(
            sums.at[jnp.minimum(block, blocks - 1)], inbox.at[n],
            near_sem.at[8], near_sem.at[n], at_z(-4 if way else 4),
        )))
    z_copies = []
    for n, (way, d) in enumerate(steps):
        z_copies.append((block_of(d), None if d == 0 else remote(
            outbox.at[n], zin.at[way, z % 4], z_sem.at[4], z_sem.at[d % 4], at_z(d),
        )))
    order = sorted(range(8), key=lambda n: -abs(steps[n][1]))

    def add_twin(p, copy):
        lo, hi = cuts[p]
        copy.wait_recv()
        for b in range(lo, hi):
            sums[b] = part[c, b] + halves[b]

    def send_near(p, r):
        for n in order:
            block, plane, near_copy = near[n]

            @pl.when(within(block, p, plane, r))
            def _(near_copy=near_copy):
                near_copy.start()

    def pass_z(p, r):
        for n in order:
            block, z_copy = z_copies[n]

            @pl.when(within(block, p, along(steps[n][1]), r))
            def _(n=n, block=block, z_copy=z_copy):
                near[n][2].wait_recv()
                both = sums[block] + inbox[n]
                if steps[n][1] == 0:
                    zin[0, z % 4] = both
                else:
                    outbox[n] = both
                    z_copy.start()

    twin0 = merge(0)

    add_twin(0, twin0)
    send_near(0, 0)
    twin1 = merge(1)
    add_twin(1, twin1)
    for p, r in [(1, 0), (0, 1), (1, 1)]:
        send_near(p, r)

    for m in range(2):
        @pl.when(raw_from[m] != z)
        def _(m=m):
            arrived(raw_row.at[pl.ds(0, 2)], raw_sem.at[1, m], twin)
        for v in range(2):
            rows = pl.ds(pl.multiple_of((v * 2 + c) * feat, 16), feat)
            remote(
                raw.at[m, rows], raw.at[m, rows], twin_sem.at[0], twin_sem.at[1], twin
            ).start()

    arrived(raw_row, twin_sem.at[1], twin)
    for m in range(2):
        got = lax.dot_general(
            pick[2 * pair + m], raw[m], (((1,), (1,)), ((), ())), preferred_element_type=F32
        ).astype(BF)
        back_out[:, m] = got.reshape(X * Y, cap, width)
    for dx, dy in plane_offs:
        to = ((x + dx) % X) * Y + (y + dy) % Y
        remote(
            back_out.at[to], back.at[x * Y + pair], bwd_sem.at[0], bwd_sem.at[1],
            at_plane(dx, dy),
        ).start()
    back[x * Y + pair] = back_out[mine]

    def columns(block, q):
        return pl.ds(pl.multiple_of(q * width + block * LANE, LANE), LANE)

    def quarter(d):
        return (along(-d)) % 4

    ag = []
    for d in range(4):
        cols = columns(jnp.minimum(my_block, blocks - 1), quarter(d))
        for dy in range(Y):
            if dy == 0:
                peer, out, sem = twin, rel_sem.at[4], rel_sem
            else:
                peer, out, sem = at_plane(0, dy), ag_sem.at[0], ag_sem
            ag.append(remote(
                emb_ref.at[:, cols], emb_ref.at[:, cols],
                out, sem.at[dy], peer,
            ))

    def gather():
        for d in range(4):
            arrived(outbox.at[pl.ds(0, 2 if d else 1)], z_sem.at[d], twin)
            cols = columns(my_block, quarter(d))
            emb_ref[:, cols] = zin[0, quarter(d)] + zin[1, quarter(d)]
            for dy in (2, 1, 3, 0):
                ag[d * Y + dy].start()

    pass_z(0, 0)
    pass_z(1, 0)
    pass_z(0, 1)
    pass_z(1, 1)
    pl.when(has_block)(gather)

    arrived(back.at[pl.ds(0, X * Y - 1)], bwd_sem.at[1], twin)
    out_ref[...] = lax.dot_general(
        hot[...], back[...].reshape(groups * cap, width), (((0,), (0,)), ((), ())),
        preferred_element_type=F32,
    ).astype(BF)

    four = emb_ref.at[:, pl.ds(0, 4 * LANE)]
    for dy in (1, 3, 2):
        from_k = 2 * ((y - dy + Y) % Y) + c
        from_block = (zl - from_k + ZL) % ZL

        @pl.when(from_block < blocks)
        def _(dy=dy, from_block=from_block):
            arrived(four, ag_sem.at[dy], twin)
            for q in range(4):
                cols = columns(from_block, q)
                remote(
                    emb_ref.at[:, cols], emb_ref.at[:, cols], rel_sem.at[4], rel_sem.at[dy], twin
                ).start()

    for dy in range(Y):
        other_k = 2 * ((y - dy + Y) % Y) + 1 - c
        other_block = (zl - other_k + ZL) % ZL

        @pl.when(other_block < blocks)
        def _(dy=dy):
            arrived(four, rel_sem.at[dy], twin)

    left(ids_all.at[pl.ds(0, groups - 1)], ids_sem.at[0], twin)
    left(raw_row.at[pl.ds(0, Y - 1)], row_sem.at[0], twin)
    for u in range(2):
        @pl.when(raw_to[u] != z)
        def _(u=u):
            left(raw_row.at[pl.ds(0, 2)], raw_sem.at[0, u], twin)
    left(raw_row, twin_sem.at[0], twin)
    for p, (lo, hi) in enumerate(cuts):
        left(rows_in.at[pl.ds(0, X * Y - 1), pl.ds(lo, hi - lo)], fwd_sem.at[0, p], twin)
    twin0.wait_send()
    twin1.wait_send()
    left(back.at[pl.ds(0, X * Y - 1)], bwd_sem.at[0], twin)
    left(outbox.at[pl.ds(0, 7)], near_sem.at[8], twin)

    @pl.when(has_block)
    def _():
        left(outbox.at[pl.ds(0, 6)], z_sem.at[4], twin)
        left(emb_ref.at[:, pl.ds(0, 12 * LANE)], ag_sem.at[0], twin)

    @pl.when(jnp.logical_not(has_block))
    def _():
        left(outbox.at[pl.ds(0, 7)], z_sem.at[4], twin)

    full = (zl + 1) % 2 != c

    @pl.when(full)
    def _():
        left(emb_ref.at[:, pl.ds(0, 16 * LANE)], rel_sem.at[4], twin)

    @pl.when(jnp.logical_not(full))
    def _():
        left(emb_ref.at[:, pl.ds(0, 12 * LANE)], rel_sem.at[4], twin)


def store(emb_ref, grad_ref, emb_out, grad_out, sem):
    copies = [
        pltpu.make_async_copy(grad_ref, grad_out, sem.at[0]),
        pltpu.make_async_copy(emb_ref, emb_out, sem.at[1]),
    ]
    for copy in copies:
        copy.start()
    for copy in copies:
        copy.wait()


def body(token_ids, table, out_grad, groups, segs):
    lines, width = table.shape
    tok, piece = out_grad.shape
    depth = segs * piece
    cap = tok // PACK
    blocks = width // LANE
    vmem = pl.BlockSpec(memory_space=pltpu.VMEM)
    hbm = pl.BlockSpec(memory_space=pltpu.HBM)
    dma = pltpu.SemaphoreType.DMA
    shapes = (
        jax.ShapeDtypeStruct((tok, depth), BF),
        jax.ShapeDtypeStruct((lines, width), BF),
    )
    emb, grad = pl.pallas_call(
        kernel,
        out_shape=shapes,
        in_specs=[hbm, hbm, hbm],
        out_specs=(vmem, vmem),
        scratch_shapes=[
            pltpu.VMEM((1, tok), jnp.int32),
            pltpu.VMEM((groups, 1, tok), jnp.int32),
            pltpu.VMEM((groups, cap, tok), jnp.int32),
            pltpu.VMEM((lines, width), BF),
            pltpu.VMEM((piece, tok), BF),
            pltpu.VMEM((Y, piece, tok), BF),
            pltpu.VMEM((2, width, tok), BF),
            pltpu.VMEM((X * Y, blocks, 2, cap, LANE), BF),
            pltpu.VMEM((X * Y, blocks, 2, cap, LANE), BF),
            pltpu.VMEM((ZL, X * Y * cap, tok), BF),
            pltpu.VMEM((ZL, tok, X * Y * cap), BF),
            pltpu.VMEM((2, blocks, tok, LANE), BF),
            pltpu.VMEM((blocks, tok, LANE), BF),
            pltpu.VMEM((blocks, tok, LANE), BF),
            pltpu.VMEM((8, tok, LANE), BF),
            pltpu.VMEM((8, tok, LANE), BF),
            pltpu.VMEM((2, 4, tok, LANE), BF),
            pltpu.VMEM((X * Y, 2, cap, width), BF),
            pltpu.VMEM((X * Y, 2, cap, width), BF),
            pltpu.VMEM((groups * cap, lines), BF),
            dma((3,)),
            dma((2,)),
            dma((2,)),
            dma((2, 2)),
            dma((2,)),
            dma((2, 2)),
            dma((2, 2)),
            dma((9,)),
            dma((5,)),
            dma((2,)),
            dma((4,)),
            dma((5,)),
        ],
        compiler_params=pltpu.CompilerParams(
            collective_id=0, has_side_effects=True, vmem_limit_bytes=50 << 20
        ),
    )(*[
        pltpu.with_memory_space_constraint(a, pltpu.HBM)
        for a in (token_ids[None, :], table, out_grad.T)
    ])
    return pl.pallas_call(
        store,
        out_shape=shapes,
        in_specs=[vmem, vmem],
        out_specs=(hbm, hbm),
        scratch_shapes=[dma((2,))],
        compiler_params=pltpu.CompilerParams(vmem_limit_bytes=50 << 20),
    )(emb, grad)


def solution(mesh):
    placed = (P("dp"), P("segment", "dp"), P("dp", "segment"))
    return jax.shard_map(
        functools.partial(body, groups=mesh.shape["dp"], segs=mesh.shape["segment"]),
        mesh=mesh,
        in_specs=placed,
        out_specs=(P("dp", None), P("segment", "dp")),
        check_vma=False,
    )
```
